1024 devices in a mesh: grp: 16 (over z_hi, y), sp: 16 (over z_lo, core), tp: 4 (over x).
Axes of the slice: x: 4, y: 4, z: 32 (z_hi: 4, z_lo: 8; z = z_hi * 8 + z_lo), core: 2. Of those that a mesh axis runs over, the one named last changes fastest.
Arguments:
- queries: bfloat16 [16, 3072, 2560], P('grp', 'sp', 'tp'), may hold values from -60 to 60
- key_tokens: bfloat16 [16, 3072, 2560], P('grp', 'sp', 'tp'), may hold values from -60 to 60
- value_tokens: bfloat16 [16, 3072, 2560], P('grp', 'sp', 'tp'), may hold values from -6 to 6
- norm_gains: float32 [2, 2560], P(None, 'grp'), may hold values from 0.25 to 1.75
- lengths: int32 [16], P('grp'), may hold values from 768 to 3072
Outputs:
- attended: bfloat16 [16, 3072, 2560], P('grp', 'sp', 'tp')
The draws below stay inside these ranges and needn't reach their ends.
All inputs are finite; a program needn't handle non-finite values.
Results may differ from the reference program's by a relative error of at most 0.011.
Values may be sent and summed in bfloat16 or wider, within the bound.
A program may use at most 64 MiB of HBM per device.

```python
import math
import jax
import jax.numpy as jnp
from jax import lax

HEADS = 20
HEAD_DIM = 128
FEATURES = 2560
LENGTH = 3072
SEQS = 16


def scaled_log(source, extent, lowest, highest):
    return jnp.exp(jax.random.uniform(source, extent, jnp.float32, math.log(lowest), math.log(highest)))


def paired_fields(key):
    full_shape = (SEQS, LENGTH, FEATURES)
    column_ramp = jnp.sqrt(1.0 + 2.0 * jnp.arange(FEATURES, dtype=jnp.float32) / (FEATURES - 1))
    query_base = jax.random.normal(jax.random.fold_in(key, 11), full_shape, jnp.float32)
    key_base = jax.random.normal(jax.random.fold_in(key, 12), full_shape, jnp.float32)
    row_scales = scaled_log(jax.random.fold_in(key, 14), (2, SEQS, LENGTH, 1), 0.3, 3.0)
    column_scales = column_ramp * scaled_log(jax.random.fold_in(key, 15), (2, 1, 1, FEATURES), 0.5, 2.0)
    query_rows = query_base * row_scales[0] * column_scales[0]
    key_rows = key_base * row_scales[1] * column_scales[1]
    return (jnp.clip(query_rows, -60.0, 60.0), jnp.clip(key_rows, -60.0, 60.0))


def draw_queries(key, part):
    return paired_fields(key)[0].astype(jnp.bfloat16)


def draw_key_tokens(key, part):
    return paired_fields(key)[1].astype(jnp.bfloat16)


def with_ends(values, key, least, top_value):
    place = [jax.random.randint(jax.random.fold_in(key, axis), (), 0, length) for axis, length in enumerate(values.shape)]
    main_axis = values.shape.index(max(values.shape))
    beside = place[:main_axis] + [(place[main_axis] + 1) % values.shape[main_axis]] + place[main_axis + 1:]
    return values.at[tuple(place)].set(least).at[tuple(beside)].set(top_value)


def block_levels(stream_key, shape, shards, least, high):
    loudness, own = 1.0, jax.random.fold_in(stream_key, 6)
    for position, blocks in shards:
        heights = jnp.exp(jax.random.uniform(jax.random.fold_in(own, position), (blocks,), jnp.float32, least / len(shards), high / len(shards)))
        loudness = loudness * jnp.repeat(heights, shape[position] // blocks).reshape([-1 if axis == position else 1 for axis in range(len(shape))])
    return loudness


def normal_values(rng, shape, scale, most, pieces=(), kind=jnp.bfloat16):
    array = jax.random.normal(rng, shape, jnp.float32) * scale
    if len(pieces) > 0:
        array = block_levels(rng, shape, pieces, -0.22, 0.18) * array
    return jnp.clip(array, min=-most, max=most).astype(kind)


def setup_inputs(seed: int = 0) -> dict:
    key_list = jax.random.split(jax.random.key(seed), 6)
    queries = draw_queries(jax.random.fold_in(key_list[5], 71), 0)
    key_tokens = draw_key_tokens(jax.random.fold_in(key_list[5], 71), 0)
    value_tokens = normal_values(key_list[2], (SEQS, LENGTH, FEATURES), 1.0, 6.0, ((0, 16), (1, 16), (2, 4)))
    norm_gains = jnp.clip(1.0 + 0.15 * jax.random.normal(key_list[3], (2, FEATURES), jnp.float32), 0.25, 1.75)
    lengths = with_ends(jax.random.randint(key_list[4], (SEQS,), LENGTH // 4, LENGTH + 1), jax.random.fold_in(key_list[4], 1), LENGTH // 4, LENGTH).astype(jnp.int32)
    return dict(queries=queries, key_tokens=key_tokens, value_tokens=value_tokens, norm_gains=norm_gains, lengths=lengths)


EPSILON = 1e-06
MASKED = -1e+30

def normalize(field, gains):
    widened = field.astype(jnp.float32)
    mean_square = lax.optimization_barrier(jnp.mean(widened * widened, axis=-1, keepdims=True))
    return (widened * lax.rsqrt(mean_square + EPSILON) * gains).astype(jnp.bfloat16)

def one_head(inputs):
    query_head, key_head, value_head, length = inputs
    scores = jnp.dot(query_head, key_head.T, preferred_element_type=jnp.float32) * (1.0 / math.sqrt(HEAD_DIM))
    visible = jnp.arange(LENGTH) < length
    scores = jnp.where(visible[None, :], scores, MASKED)
    largest = lax.optimization_barrier(jnp.max(scores, axis=-1, keepdims=True))
    weights = jnp.where(visible[None, :], jnp.exp(scores - largest), 0.0)
    denominator = lax.optimization_barrier(jnp.sum(weights, axis=-1, keepdims=True))
    numerator = jnp.dot(weights.astype(jnp.bfloat16), value_head, preferred_element_type=jnp.float32)
    return numerator / denominator

def by_heads(field):
    return field.reshape(LENGTH, HEADS, HEAD_DIM).transpose(1, 0, 2)

def one_sample(inputs):
    query_sample, key_sample, value_sample, length = inputs
    counts = jnp.broadcast_to(length, (HEADS,))
    result = lax.map(one_head, (by_heads(query_sample), by_heads(key_sample), by_heads(value_sample), counts))
    return result.transpose(1, 0, 2).reshape(LENGTH, FEATURES).astype(jnp.bfloat16)

def reference(queries, key_tokens, value_tokens, norm_gains, lengths):
    query_norm = normalize(queries, norm_gains[0])
    key_norm = normalize(key_tokens, norm_gains[1])
    return lax.map(one_sample, (query_norm, key_norm, value_tokens, lengths))
```

```python
import functools
import math

import jax
import jax.numpy as jnp
from jax import lax
from jax.experimental import pallas as pl
from jax.experimental.pallas import tpu as pltpu
from jax.sharding import PartitionSpec as P

HEAD_DIM = 128
EPSILON = 1e-06
MASKED = -1e30
MESH = pl.DeviceIdType.MESH

OWNERS = (1, 2, 3, 5, 6)
HEAD_ORDER = (2, 0, 4, 1, 3)
CHIPS = 8


def near_to_far(chip):
    return sorted(range(CHIPS), key=lambda other: (abs(other - chip), other))


def pick(index, choices, default):
    value = jnp.int32(default)
    for key, choice in choices:
        value = jnp.where(index == key, jnp.int32(choice), value)
    return value


def attention_kernel(
    sizes,
    length_ref,
    q_ref,
    k_ref,
    v_ref,
    gains_ref,
    out_ref,
    q_buf,
    k_buf,
    v_buf,
    k_norm,
    scale_buf,
    part_buf,
    gains_buf,
    gain_row,
    score_ref,
    o_buf,
    send_q,
    send_k,
    send_v,
    send_s,
    send_p,
    send_g,
    send_f,
    send_o,
    recv_q,
    recv_k,
    recv_v,
    recv_s,
    recv_p,
    recv_g,
    recv_o,
):
    groups, tensors, full_width = sizes
    rows, width = q_ref.shape
    slices = gains_buf.shape[0]
    piece = gains_ref.shape[1]
    group = lax.axis_index("grp")
    me = lax.axis_index("sp")
    column = lax.axis_index("tp")
    chip = me // 2
    side = me % 2
    partner = me + 1 - 2 * side
    gives_gains = (group // slices) == column
    my_slice = group % slices
    owner = functools.reduce(jnp.logical_or, [chip == c for c in OWNERS])
    head = pick(chip, [(c, h) for h, c in enumerate(OWNERS)], 0)
    columns = pl.ds(pl.multiple_of(head * HEAD_DIM, HEAD_DIM), HEAD_DIM)

    barrier = pltpu.get_barrier_semaphore()
    for step in range(1, CHIPS):
        pl.semaphore_signal(
            barrier,
            inc=1,
            device_id={"sp": lax.rem(chip + step, CHIPS) * 2 + side},
            device_id_type=MESH,
        )
    pl.semaphore_signal(barrier, inc=1, device_id={"sp": partner}, device_id_type=MESH)
    for step in range(1, tensors):
        pl.semaphore_signal(
            barrier,
            inc=1,
            device_id={"tp": lax.rem(column + step, tensors)},
            device_id_type=MESH,
        )
    for y in range(slices):
        source = column * slices + y

        @pl.when(source != group)
        def _():
            pl.semaphore_signal(barrier, inc=1, device_id={"grp": source}, device_id_type=MESH)

    ones = jnp.ones((8, width), jnp.bfloat16)
    for place, ref in enumerate((q_ref, k_ref)):
        wide = ref[...].astype(jnp.float32)
        square = wide * wide
        high = square.astype(jnp.bfloat16)
        low = (square - high.astype(jnp.float32)).astype(jnp.bfloat16)
        over = (((1,), (1,)), ((), ()))
        total = lax.dot_general(ones, high, over, preferred_element_type=jnp.float32)
        total = total + lax.dot_general(ones, low, over, preferred_element_type=jnp.float32)
        part_buf[pl.ds(column, 1), pl.ds(place, 1), :] = total[None, 0:1, :]

    near = CHIPS - 1 + 1 + tensors - 1
    pl.semaphore_wait(barrier, near + jnp.where(gives_gains, groups - 1, 0))

    def block_copies(h):
        lanes = pl.ds(h * HEAD_DIM, HEAD_DIM)
        target = {"sp": OWNERS[h] * 2 + side}
        return [
            pltpu.make_async_remote_copy(
                src_ref=q_ref.at[:, lanes],
                dst_ref=q_buf.at[chip],
                send_sem=send_q.at[h],
                recv_sem=recv_q.at[chip],
                device_id=target,
                device_id_type=MESH,
            ),
            pltpu.make_async_remote_copy(
                src_ref=k_ref.at[:, lanes],
                dst_ref=k_buf.at[me],
                send_sem=send_k.at[h],
                recv_sem=recv_k.at[me],
                device_id=target,
                device_id_type=MESH,
            ),
            pltpu.make_async_remote_copy(
                src_ref=v_ref.at[:, lanes],
                dst_ref=v_buf.at[me],
                send_sem=send_v.at[h],
                recv_sem=recv_v.at[me],
                device_id=target,
                device_id_type=MESH,
            ),
        ]

    def scale_copy(h):
        return pltpu.make_async_remote_copy(
            src_ref=scale_buf.at[me],
            dst_ref=scale_buf.at[me],
            send_sem=send_s.at[h],
            recv_sem=recv_s.at[me],
            device_id={"sp": OWNERS[h] * 2 + side},
            device_id_type=MESH,
        )

    def part_copy(step):
        return pltpu.make_async_remote_copy(
            src_ref=part_buf.at[column],
            dst_ref=part_buf.at[column],
            send_sem=send_p.at[step],
            recv_sem=recv_p.at[column],
            device_id={"tp": lax.rem(column + step, tensors)},
            device_id_type=MESH,
        )

    def gain_copy(step):
        return pltpu.make_async_remote_copy(
            src_ref=gains_ref,
            dst_ref=gains_buf.at[my_slice],
            send_sem=send_g.at[step],
            recv_sem=recv_g.at[my_slice],
            device_id={"grp": lax.rem(group + step, groups)},
            device_id_type=MESH,
        )

    def forward_copies(block, k_from, v_from):
        trips = (
            (k_from, k_buf, recv_k),
            (v_from, v_buf, recv_v),
            (scale_buf.at[block], scale_buf, recv_s),
        )
        return [
            pltpu.make_async_remote_copy(
                src_ref=source,
                dst_ref=into.at[block],
                send_sem=send_f.at[place, block // 2],
                recv_sem=landing.at[block],
                device_id={"sp": partner},
                device_id_type=MESH,
            )
            for place, (source, into, landing) in enumerate(trips)
        ]

    for step in range(1, tensors):
        part_copy(step).start()

    @pl.when(gives_gains)
    def _():
        for step in range(1, groups):
            gain_copy(step).start()

    for h in HEAD_ORDER:

        @pl.when(chip != OWNERS[h])
        def _():
            for copy in block_copies(h):
                copy.start()

    for step in range(1, tensors):
        other = lax.rem(column + step, tensors)
        pltpu.make_async_remote_copy(
            src_ref=part_buf.at[column],
            dst_ref=part_buf.at[other],
            send_sem=send_p.at[step],
            recv_sem=recv_p.at[other],
            device_id={"tp": other},
            device_id_type=MESH,
        ).wait_recv()
    sums = part_buf[0]
    for t in range(1, tensors):
        sums = sums + part_buf[t]
    scale_buf[pl.ds(me, 1)] = lax.rsqrt(sums / full_width + EPSILON)[None]
    for h in HEAD_ORDER:

        @pl.when(chip != OWNERS[h])
        def _():
            scale_copy(h).start()

    def own_forwards():
        return forward_copies(me, k_ref.at[:, columns], v_ref.at[:, columns])

    def passed_forwards(block):
        return forward_copies(block, k_buf.at[block], v_buf.at[block])

    def scale_column(block, place):
        row = scale_buf[block][place : place + 1, :]
        diagonal = lax.broadcasted_iota(jnp.int32, (rows, rows), 0) == lax.broadcasted_iota(
            jnp.int32, (rows, rows), 1
        )
        spread = jnp.where(diagonal, jnp.broadcast_to(row, (rows, rows)), 0.0)
        return jnp.sum(spread, axis=1, keepdims=True)

    @pl.when(owner)
    def _():
        for copy in own_forwards():
            copy.start()

        q_buf[pl.ds(chip, 1)] = q_ref[:, columns][None]
        k_buf[pl.ds(me, 1)] = k_ref[:, columns][None]
        v_buf[pl.ds(me, 1)] = v_ref[:, columns][None]

    @pl.when(gives_gains)
    def _():
        gains_buf[pl.ds(my_slice, 1)] = gains_ref[...][None]

    for y in range(slices):
        source = column * slices + y

        @pl.when(source != group)
        def _():
            pltpu.make_async_remote_copy(
                src_ref=gains_ref,
                dst_ref=gains_buf.at[y],
                send_sem=send_g.at[0],
                recv_sem=recv_g.at[y],
                device_id={"grp": source},
                device_id_type=MESH,
            ).wait_recv()

    for y in range(slices):
        gain_row[:, y * piece : (y + 1) * piece] = gains_buf[y]

    @pl.when(owner)
    def _():
        gains = gain_row[:, columns]
        query_gain = gains[0:1, :]
        key_gain = gains[1:2, :]

        def normalize_key(block):
            wide = k_buf[block].astype(jnp.float32)
            k_norm[pl.ds(block, 1)] = (wide * scale_column(block, 1) * key_gain).astype(
                jnp.bfloat16
            )[None]

        def landed(block):
            for buf, sem in ((k_buf, recv_k), (v_buf, recv_v), (scale_buf, recv_s)):
                pltpu.make_async_remote_copy(
                    src_ref=buf.at[block],
                    dst_ref=buf.at[block],
                    send_sem=send_f.at[0, 0],
                    recv_sem=sem.at[block],
                    device_id={"sp": partner},
                    device_id_type=MESH,
                ).wait_recv()

        normalize_key(me)
        landed(partner)
        normalize_key(partner)

        order = pick(
            chip,
            [
                (c, sum(o * CHIPS**i for i, o in enumerate(near_to_far(c)[1:])))
                for c in OWNERS
            ],
            0,
        )

        def arrive(step, left):
            there = lax.rem(left, CHIPS)
            block = there * 2 + side
            landed(block)
            for copy in passed_forwards(block):
                copy.start()
            normalize_key(block)
            other = there * 2 + 1 - side
            landed(other)
            normalize_key(other)
            pltpu.make_async_remote_copy(
                src_ref=q_buf.at[there],
                dst_ref=q_buf.at[there],
                send_sem=send_q.at[0],
                recv_sem=recv_q.at[there],
                device_id={"sp": partner},
                device_id_type=MESH,
            ).wait_recv()
            return left // CHIPS

        lax.fori_loop(0, CHIPS - 1, arrive, order)

        length = length_ref[0]
        factor = math.log2(math.e) / math.sqrt(HEAD_DIM)
        span = 2 * rows

        def attend(there):
            wide = q_buf[there].astype(jnp.float32)
            query = (wide * scale_column(there * 2 + side, 0) * query_gain * factor).astype(
                jnp.bfloat16
            )
            best = None
            for c in range(CHIPS):
                keys = k_norm[2 * c : 2 * c + 2].reshape(span, HEAD_DIM)
                scores = lax.dot_general(
                    query, keys, (((1,), (1,)), ((), ())), preferred_element_type=jnp.float32
                )
                place = lax.broadcasted_iota(jnp.int32, (1, span), 1) + c * span
                scores = scores + jnp.where(place < length, 0.0, MASKED)
                score_ref[:, c * span : (c + 1) * span] = scores
                highest = jnp.max(scores, axis=1, keepdims=True)
                best = highest if best is None else jnp.maximum(best, highest)
            total = None
            numerator = None
            for c in range(CHIPS):
                weights = jnp.exp2(score_ref[:, c * span : (c + 1) * span] - best)
                part = jnp.sum(weights, axis=1, keepdims=True)
                values = v_buf[2 * c : 2 * c + 2].reshape(span, HEAD_DIM)
                update = jnp.dot(
                    weights.astype(jnp.bfloat16), values, preferred_element_type=jnp.float32
                )
                total = part if total is None else total + part
                numerator = update if numerator is None else numerator + update
            return (numerator / total).astype(jnp.bfloat16)

        def result_copy(there):
            return pltpu.make_async_remote_copy(
                src_ref=o_buf.at[there],
                dst_ref=out_ref.at[:, columns],
                send_sem=send_o.at[there],
                recv_sem=recv_o.at[head],
                device_id={"sp": there * 2 + side},
                device_id_type=MESH,
            )

        backward = pick(
            chip,
            [
                (c, sum(o * CHIPS**i for i, o in enumerate(near_to_far(c)[:0:-1])))
                for c in OWNERS
            ],
            0,
        )

        def answer(step, left):
            there = lax.rem(left, CHIPS)
            o_buf[pl.ds(there, 1)] = attend(there)[None]
            result_copy(there).start()
            return left // CHIPS

        lax.fori_loop(0, CHIPS - 1, answer, backward)
        out_ref[:, columns] = attend(chip)

        for step in range(1, CHIPS):
            result_copy(lax.rem(chip + step, CHIPS)).wait_send()
            for copy in passed_forwards(lax.rem(chip + step, CHIPS) * 2 + side):
                copy.wait_send()
        for copy in own_forwards():
            copy.wait_send()

    for h in HEAD_ORDER:

        @pl.when(chip != OWNERS[h])
        def _():
            for copy in block_copies(h):
                copy.wait_send()
            scale_copy(h).wait_send()
            lanes = pl.ds(h * HEAD_DIM, HEAD_DIM)
            pltpu.make_async_remote_copy(
                src_ref=out_ref.at[:, lanes],
                dst_ref=out_ref.at[:, lanes],
                send_sem=send_o.at[0],
                recv_sem=recv_o.at[h],
                device_id={"sp": OWNERS[h] * 2 + side},
                device_id_type=MESH,
            ).wait_recv()

    for step in range(1, tensors):
        part_copy(step).wait_send()

    @pl.when(gives_gains)
    def _():
        for step in range(1, groups):
            gain_copy(step).wait_send()


def per_device(sizes, queries, key_tokens, value_tokens, norm_gains, lengths):
    groups, tensors, _ = sizes
    rows, width = queries.shape[1:]
    heads = width // HEAD_DIM
    piece = norm_gains.shape[1]
    slices = width // piece
    blocks = 2 * CHIPS
    vmem = pl.BlockSpec(memory_space=pltpu.VMEM)
    dma = pltpu.SemaphoreType.DMA
    out = pl.pallas_call(
        functools.partial(attention_kernel, sizes),
        out_shape=jax.ShapeDtypeStruct((rows, width), jnp.bfloat16),
        in_specs=[pl.BlockSpec(memory_space=pltpu.SMEM)] + [vmem] * 4,
        out_specs=vmem,
        scratch_shapes=[
            pltpu.VMEM((CHIPS, rows, HEAD_DIM), jnp.bfloat16),
            pltpu.VMEM((blocks, rows, HEAD_DIM), jnp.bfloat16),
            pltpu.VMEM((blocks, rows, HEAD_DIM), jnp.bfloat16),
            pltpu.VMEM((blocks, rows, HEAD_DIM), jnp.bfloat16),
            pltpu.VMEM((blocks, 2, rows), jnp.float32),
            pltpu.VMEM((tensors, 2, rows), jnp.float32),
            pltpu.VMEM((slices, 2, piece), jnp.float32),
            pltpu.VMEM((2, width), jnp.float32),
            pltpu.VMEM((rows, blocks * rows), jnp.float32),
            pltpu.VMEM((CHIPS, rows, HEAD_DIM), jnp.bfloat16),
            dma((heads,)),
            dma((heads,)),
            dma((heads,)),
            dma((heads,)),
            dma((max(tensors, 2),)),
            dma((max(groups, 2),)),
            dma((3, CHIPS)),
            dma((CHIPS,)),
            dma((CHIPS,)),
            dma((blocks,)),
            dma((blocks,)),
            dma((blocks,)),
            dma((max(tensors, 2),)),
            dma((slices,)),
            dma((heads,)),
        ],
        compiler_params=pltpu.CompilerParams(
            collective_id=0, has_side_effects=True, vmem_limit_bytes=48 * 1024 * 1024
        ),
    )(lengths, queries[0], key_tokens[0], value_tokens[0], norm_gains)
    return out[None]


def solution(mesh):
    placed = (
        P("grp", "sp", "tp"),
        P("grp", "sp", "tp"),
        P("grp", "sp", "tp"),
        P(None, "grp"),
        P("grp"),
    )
    groups, tensors = mesh.shape["grp"], mesh.shape["tp"]
    sizes = (groups, tensors, 5 * HEAD_DIM * tensors)
    return jax.shard_map(
        functools.partial(per_device, sizes),
        mesh=mesh,
        in_specs=placed,
        out_specs=P("grp", "sp", "tp"),
        check_vma=False,
    )
```
